32 devices in a mesh: row: 4 (over y, core), col: 8 (over z, x).
Axes of the slice: x: 2, y: 2, z: 4, core: 2. Of those that a mesh axis runs over, the one named last changes fastest.
Arguments:
- covariance: float32 [16384, 16384], P('row', 'col'), as said below
- weights: float32 [16384], P(('row', 'col')), may hold values from 0.5 to 1
- dual_slacks: float32 [16384], P(('row', 'col')), may hold values from 2.5 to 10
- returns: float32 [16384], P(('row', 'col')), may hold values from -6 to 6
- targets: float32 [256], P('col'), may hold values from 0.5 to 1
- sector_duals: float32 [256], replicated, may hold values from -6 to 6
- lengths: int32 [256], replicated, may hold values from 1 to 1024, 16384 in all
Outputs:
- factored: float32 [16384, 16384], P('row', 'col')
- solved_rhs: float32 [16384], P('row')
- sector_cols: float32 [16384, 256], P('row', 'col')
- sector_resid: float32 [256], P('col')
The draws below stay inside these ranges and needn't reach their ends.
Inputs may be any that keep to these rules, and one draw needn't show every extreme that they name: `lengths`: lengths sum to 16384. `covariance`: only the lower triangle with the diagonal is read; with the added diagonal the system is positive definite.
All inputs are finite; a program needn't handle non-finite values.
Results may differ from the reference program's by a relative error of at most 0.0003.
Values sent between devices are 32-bit elements; how exact they have to be, the bound alone decides.
A program may use at most 192 MiB of HBM per device.

```python
import math
import jax
import jax.numpy as jnp
import numpy as np
from jax import lax

N = 16384
SECT = 256
MOST_LEN = 1024
NB = 128
PANELS = 8


def draw_covariance(key, part):
    factor_count = max(4, min(64, N // 32))
    key_load, key_beta, key_noise = jax.random.split(key, 3)
    loadings = jnp.clip(jax.random.normal(key_load, (N, factor_count), jnp.float32), -4.0, 4.0)
    noise = jnp.clip(jax.random.normal(key_noise, (N, N), jnp.float32), -4.0, 4.0)
    market = 1.0
    betas = jax.random.uniform(key_beta, (N,), jnp.float32, 0.5, 1.5)
    scaled = loadings
    factor_part = jnp.dot(scaled, scaled.T, precision=lax.Precision.HIGHEST) * (0.5 / factor_count)
    market_part = market / N * betas[:, None] * betas[None, :]
    return factor_part + market_part + noise * (1.0 / math.sqrt(N))


def levels(rng, dims, pieces, smallest, high):
    factor_of, own = 1.0, jax.random.fold_in(rng, 6)
    for position, shards_of in pieces:
        steps = jnp.exp(jax.random.uniform(jax.random.fold_in(own, position), (shards_of,), jnp.float32, smallest / len(pieces), high / len(pieces)))
        factor_of = factor_of * jnp.repeat(steps, dims[position] // shards_of).reshape([-1 if axis == position else 1 for axis in range(len(dims))])
    return factor_of


def profile(count, total, reach, slope):
    loads = [(1 << 20) // math.isqrt(standing ** slope) + 1 for standing in range(2, count + 1)]
    spare, counts = total - reach - (count - 1), [1] * (count - 1)
    while spare > 0:
        candidates = [i for i in range(count - 1) if counts[i] < reach]
        mass, left = sum([loads[i] for i in candidates]), spare
        for i in candidates:
            more = min(reach - counts[i], max(1, left * loads[i] // mass), spare)
            counts[i] = counts[i] + more
            spare = spare - more
    return np.array([reach] + counts)


def uneven_parts(key, amount, total, most, skew):
    if amount == 2:
        one = jax.random.randint(key, (), max(1, total - most), min(most, total - 1) + 1)
        return jnp.stack([one, total - one])
    sizes = jnp.asarray(profile(amount, total, most, skew), jnp.int32)
    couples = (amount - 1) // 2
    giver, receiver = sizes[1:1 + 2 * couples:2], sizes[2:2 + 2 * couples:2]
    margin = jnp.minimum(giver - 1, most - receiver)
    moved = jax.random.randint(jax.random.fold_in(key, 1), (couples,), 0, 1 << 20) % (margin + 1)
    sizes = sizes.at[1:1 + 2 * couples:2].set(giver - moved).at[2:2 + 2 * couples:2].set(receiver + moved)
    return sizes[jax.random.permutation(jax.random.fold_in(key, 2), amount)]


def centred(stream_key, shape, spread, reach, cuts=(), held_as=jnp.bfloat16):
    gain = levels(stream_key, shape, cuts, -0.22, 0.18) if cuts else 1.0
    entries = jax.random.normal(stream_key, shape, jnp.float32) * spread * gain
    return jnp.minimum(jnp.maximum(entries, -reach), reach).astype(held_as)


def setup_inputs(seed: int = 0) -> dict:
    key_of = jax.random.split(jax.random.key(seed), 8)
    covariance = draw_covariance(jax.random.fold_in(key_of[7], 71), 0)
    weights = jnp.clip(jnp.exp(math.log(1.0) - 0.6931472 * jax.random.uniform(key_of[1], (N,), jnp.float32) ** levels(key_of[1], (N,), ((0, 32),), -0.2, 0.2)), 0.5, 1.0)
    dual_slacks = jnp.clip(jnp.exp(math.log(10.0) - 1.3862944 * jax.random.uniform(key_of[2], (N,), jnp.float32) ** levels(key_of[2], (N,), ((0, 32),), -0.2, 0.2)), 2.5, 10.0)
    returns = centred(key_of[3], (N,), 1.0, 6.0, ((0, 32),), jnp.float32)
    targets = jnp.clip(0.5 + 0.5 * jax.random.uniform(key_of[4], (SECT,), jnp.float32) ** levels(key_of[4], (SECT,), ((0, 8),), -0.2, 0.2), 0.5, 1.0)
    sector_duals = centred(key_of[5], (SECT,), 1.0, 6.0, (), jnp.float32)
    lengths = uneven_parts(key_of[6], SECT, N, MOST_LEN, 2).astype(jnp.int32)
    return dict(covariance=covariance, weights=weights, dual_slacks=dual_slacks, returns=returns, targets=targets, sector_duals=sector_duals, lengths=lengths)


HIGH = lax.Precision.HIGHEST
SIGMA_GAP = 0.5

def symmetric_product(covariance, weights):
    blocks = 16
    rows_per = covariance.shape[0] // blocks
    stacked = covariance.reshape(blocks, rows_per, covariance.shape[1])
    columns = jnp.arange(covariance.shape[1], dtype=jnp.int32)
    starts = jnp.arange(blocks, dtype=jnp.int32) * rows_per

    def accumulate(column_sum, item):
        tile_block, start_row = item
        row_index = start_row + jnp.arange(rows_per, dtype=jnp.int32)
        lower_part = jnp.where(row_index[:, None] >= columns[None, :], tile_block, 0.0)
        strict = jnp.where(row_index[:, None] > columns[None, :], tile_block, 0.0)
        weight_rows = lax.dynamic_slice_in_dim(weights, start_row, rows_per)
        column_sum = column_sum + jnp.dot(weight_rows, strict, precision=HIGH)
        return (column_sum, jnp.dot(lower_part, weights, precision=HIGH))
    column_sum, row_parts = lax.scan(accumulate, jnp.zeros((covariance.shape[1],), jnp.float32), (stacked, starts))
    return column_sum + row_parts.reshape(-1)

def reference(covariance, weights, dual_slacks, returns, targets, sector_duals, lengths):
    sector_ends = jnp.cumsum(lengths).astype(jnp.int32)
    offsets = sector_ends - lengths
    assets = jnp.arange(N, dtype=jnp.int32)
    member = ((assets[:, None] >= offsets[None, :]) & (assets[:, None] < sector_ends[None, :])).astype(jnp.float32)
    sector_sizes = lengths.astype(jnp.float32)
    sector_resid = targets - jnp.dot(weights, member, precision=HIGH) / sector_sizes
    mean_gap = jnp.sum(weights * dual_slacks) / N
    product = symmetric_product(covariance, weights)
    prices = jnp.dot(member, sector_duals, precision=HIGH)
    rhs = returns - product - prices + SIGMA_GAP * mean_gap / weights
    extras = jnp.concatenate([rhs[:, None], member / jnp.sqrt(sector_sizes)[None, :]], axis=1)
    split = PANELS * NB
    diag_term = dual_slacks / weights
    head = covariance[:split, :split]
    head_index = jnp.arange(split, dtype=jnp.int32)
    head_lower = jnp.tril(head).at[head_index, head_index].add(diag_term[:split])
    head_sym = head_lower + jnp.tril(head, -1).T
    factor_head = jnp.linalg.cholesky(head_sym)
    inverse_head = lax.linalg.triangular_solve(factor_head, jnp.eye(split, dtype=jnp.float32), left_side=True, lower=True)
    factor_tail = jnp.dot(covariance[split:, :split], inverse_head.T, precision=HIGH)
    tail_index = jnp.arange(N - split, dtype=jnp.int32)
    schur = covariance[split:, split:] - jnp.dot(factor_tail, factor_tail.T, precision=HIGH)
    schur = schur.at[tail_index, tail_index].add(diag_term[split:])
    solved_head = jnp.dot(inverse_head, extras[:split], precision=HIGH)
    solved_tail = extras[split:] - jnp.dot(factor_tail, solved_head, precision=HIGH)
    top = jnp.concatenate([jnp.tril(factor_head), jnp.zeros((split, N - split), jnp.float32)], axis=1)
    bottom = jnp.concatenate([factor_tail, jnp.tril(schur)], axis=1)
    factored = jnp.concatenate([top, bottom], axis=0)
    solved = jnp.concatenate([solved_head, solved_tail], axis=0)
    return (factored, solved[:, 0], solved[:, 1:], sector_resid)
```

```python
import functools

import jax
import jax.numpy as jnp
from jax import lax
from jax.experimental import pallas as pl
from jax.experimental.pallas import tpu as pltpu
from jax.sharding import PartitionSpec as P

NB = 128
PANELS = 8
CHUNKS = 64
SLACK = 2
AHEAD = 16

HIGHEST = lax.Precision.HIGHEST
HIGH = lax.Precision.HIGH
SIGMA_GAP = 0.5
NT = (((1,), (1,)), ((), ()))
MESH = pl.DeviceIdType.MESH
VMEM = pl.BlockSpec(memory_space=pltpu.VMEM)
ANY = pl.BlockSpec(memory_space=pl.ANY)


def eliminate(block):
    width = block.shape[0]
    rows = lax.broadcasted_iota(jnp.int32, (width, width), 0)
    lanes = lax.broadcasted_iota(jnp.int32, (width, width), 1)

    def step(j, carry):
        left, right = carry
        at_row = rows == j
        row = jnp.sum(jnp.where(at_row, left, 0.0), axis=0, keepdims=True)
        other = jnp.sum(jnp.where(at_row, right, 0.0), axis=0, keepdims=True)
        column = jnp.sum(jnp.where(lanes == j, left, 0.0), axis=1, keepdims=True)
        pivot = jnp.sum(jnp.where(lanes[:1] == j, row, 0.0), axis=1, keepdims=True)
        scale = lax.rsqrt(pivot)
        scale = scale * (1.5 - 0.5 * pivot * scale * scale)
        row = row * scale
        other = other * scale
        column = column * scale
        below = rows > j
        left = jnp.where(below, left - column * row, jnp.where(at_row, row, left))
        right = jnp.where(below, right - column * other, jnp.where(at_row, other, right))
        return (left, right)

    identity = (rows == lanes).astype(jnp.float32)
    upper, inverse = lax.fori_loop(0, width, step, (block, identity))
    upper = jnp.where(lanes >= rows, upper, 0.0)
    return (upper.T, inverse)


def factor_panel(factor_ref, inverse_ref, first):
    order = factor_ref.shape[0]
    last = first + NB
    here = slice(first, last)
    lower, inverse = eliminate(factor_ref[here, here])
    factor_ref[here, here] = lower
    inverse_ref[here, here] = inverse
    if first:
        done = jnp.dot(
            factor_ref[here, :first], inverse_ref[:first, :first], precision=HIGHEST,
            preferred_element_type=jnp.float32,
        )
        inverse_ref[here, :first] = -jnp.dot(
            inverse, done, precision=HIGHEST, preferred_element_type=jnp.float32
        )
    if last < order:
        below = lax.dot_general(
            factor_ref[last:, here], inverse, NT, precision=HIGHEST,
            preferred_element_type=jnp.float32,
        )
        factor_ref[last:, here] = below
        factor_ref[here, last:] = jnp.zeros((NB, order - last), jnp.float32)
        for top in range(last, order, NB):
            factor_ref[top:, top:top + NB] -= lax.dot_general(
                below[top - last:], below[top - last:top - last + NB], NT,
                precision=HIGHEST, preferred_element_type=jnp.float32,
            )


def gather_kernel(row_devices, col_devices, mine_ref, all_ref, send_sem, recv_sem):
    count = row_devices * col_devices
    me = lax.axis_index("row") * col_devices + lax.axis_index("col")
    all_ref[me] = mine_ref[...]

    def copy(k):
        target = lax.rem(me + k, count)
        return pltpu.make_async_remote_copy(
            src_ref=mine_ref, dst_ref=all_ref.at[me], send_sem=send_sem.at[k],
            recv_sem=recv_sem.at[k],
            device_id=(target // col_devices, lax.rem(target, col_devices)),
            device_id_type=MESH,
        )

    def start(k, carry):
        copy(k).start()
        return carry

    def finish(k, carry):
        copy(k).wait_recv()
        copy(k).wait_send()
        return carry

    lax.fori_loop(1, count, start, 0)
    lax.fori_loop(1, count, finish, 0)


def gather_small(mine, row_devices, col_devices):
    count = row_devices * col_devices
    return pl.pallas_call(
        functools.partial(gather_kernel, row_devices, col_devices),
        out_shape=jax.ShapeDtypeStruct((count,) + mine.shape, jnp.float32),
        in_specs=[VMEM],
        out_specs=VMEM,
        scratch_shapes=[pltpu.SemaphoreType.DMA((count,)), pltpu.SemaphoreType.DMA((count,))],
        compiler_params=pltpu.CompilerParams(has_side_effects=True),
        cost_estimate=pl.CostEstimate(flops=10**9, bytes_accessed=10**6, transcendentals=0),
    )(mine)


def sum_kernel(
    row_devices, col_devices, per_col, row_ref, col_ref, all_ref, inbox, mine, send_sem,
    recv_sem, send_back, recv_back,
):
    count = row_devices * col_devices
    row, col = lax.axis_index("row"), lax.axis_index("col")
    me = row * col_devices + col

    def to_row(s):
        return pltpu.make_async_remote_copy(
            src_ref=row_ref.at[s], dst_ref=inbox.at[col], send_sem=send_sem.at[s],
            recv_sem=recv_sem.at[col], device_id=(row, s), device_id_type=MESH,
        )

    def to_col(t):
        target = col * per_col + t
        return target, pltpu.make_async_remote_copy(
            src_ref=col_ref.at[t], dst_ref=inbox.at[col_devices + row],
            send_sem=send_sem.at[col_devices + t], recv_sem=recv_sem.at[col_devices + row],
            device_id=(target // col_devices, lax.rem(target, col_devices)),
            device_id_type=MESH,
        )

    def arrival(slot):
        return pltpu.make_async_remote_copy(
            src_ref=inbox.at[slot], dst_ref=inbox.at[slot], send_sem=send_sem.at[0],
            recv_sem=recv_sem.at[slot], device_id=(row, col), device_id_type=MESH,
        )

    inbox[col] = row_ref[col]
    for s in range(col_devices):
        @pl.when(s != col)
        def _():
            to_row(s).start()
    for t in range(per_col):
        target, copy = to_col(t)

        @pl.when(target != me)
        def _():
            copy.start()

        @pl.when(target == me)
        def _():
            inbox[col_devices + row] = col_ref[t]
    source_col = me // per_col
    for s in range(col_devices):
        @pl.when(s != col)
        def _():
            arrival(s).wait_recv()
    for q in range(row_devices):
        @pl.when(q * col_devices + source_col != me)
        def _():
            arrival(col_devices + q).wait_recv()
    total = inbox[0]
    for slot in range(1, col_devices + row_devices):
        total = total + inbox[slot]
    mine[...] = total
    all_ref[me] = total

    def back(k):
        target = lax.rem(me + k, count)
        return pltpu.make_async_remote_copy(
            src_ref=mine, dst_ref=all_ref.at[me], send_sem=send_back.at[k],
            recv_sem=recv_back.at[k],
            device_id=(target // col_devices, lax.rem(target, col_devices)),
            device_id_type=MESH,
        )

    def start(k, carry):
        back(k).start()
        return carry

    def finish(k, carry):
        back(k).wait_recv()
        back(k).wait_send()
        return carry

    lax.fori_loop(1, count, start, 0)
    lax.fori_loop(1, count, finish, 0)
    for s in range(col_devices):
        @pl.when(s != col)
        def _():
            to_row(s).wait_send()
    for t in range(per_col):
        target, copy = to_col(t)

        @pl.when(target != me)
        def _():
            copy.wait_send()


def sum_parts(row_part, col_part, row_devices, col_devices):
    count = row_devices * col_devices
    piece = row_part.shape[0] // col_devices
    per_col = col_part.shape[0] // piece
    dma = pltpu.SemaphoreType.DMA
    return pl.pallas_call(
        functools.partial(sum_kernel, row_devices, col_devices, per_col),
        out_shape=jax.ShapeDtypeStruct((count, 1, piece), jnp.float32),
        in_specs=[VMEM, VMEM],
        out_specs=VMEM,
        scratch_shapes=[
            pltpu.VMEM((col_devices + row_devices, 1, piece), jnp.float32),
            pltpu.VMEM((1, piece), jnp.float32),
            dma((col_devices + per_col,)),
            dma((col_devices + row_devices,)),
            dma((count,)),
            dma((count,)),
        ],
        compiler_params=pltpu.CompilerParams(has_side_effects=True),
        cost_estimate=pl.CostEstimate(flops=10**9, bytes_accessed=10**6, transcendentals=0),
    )(row_part.reshape(col_devices, 1, piece), col_part.reshape(per_col, 1, piece)).reshape(-1)


def spread_kernel(
    row_devices, col_devices, width, cov_ref, diag_ref, rows_out, cols_out, factor_out,
    inverse_out, rows, cols, factor, inverse, local_sem, row_send, row_recv, col_send,
    col_recv, head_send, head_recv, down_send, down_recv,
):
    tile_rows, lead = rows.shape
    depth = col_devices // width
    half = tile_rows // 2
    step_rows = half // CHUNKS
    part = NB // 2
    row, col = lax.axis_index("row"), lax.axis_index("col")
    z, x = col // width, lax.rem(col, width)
    owner = col // 2
    side = lax.rem(col, 2)
    is_source = col == 0
    is_root = is_source & (row == 0)

    links = (
        (
            ((z == 0) & (x + 1 < width), col + 1),
            ((x >= 1) & (z + 1 < depth), col + width),
            ((z >= 1) & (x == 1), col - 1),
        ),
        (
            ((x == 0) & (z + 1 < depth), col + width),
            ((z >= 1) & (x + 1 < width), col + 1),
            ((z == 1) & (x >= 1), col - width),
        ),
    )
    hops = (
        jnp.where(x >= 1, x + z, jnp.where(z >= 1, z + 2, 0)),
        jnp.where(z >= 1, x + z, jnp.where(x >= 1, x + 2, 0)),
    )
    chain_hops = jnp.where(side == 0, hops[0], hops[1])

    def row_slice(tree, i):
        return pl.ds(pl.multiple_of(tree * half + i * step_rows, step_rows), step_rows)

    def row_copy(tree, link, i, source):
        here = row_slice(tree, i)
        origin = cov_ref.at[here, pl.ds(0, lead)] if source else rows.at[here]
        return pltpu.make_async_remote_copy(
            src_ref=origin, dst_ref=rows.at[here], send_sem=row_send.at[tree, link],
            recv_sem=row_recv.at[tree, i], device_id=(row, links[tree][link][1]),
            device_id_type=MESH,
        )

    def col_copy(i, origin):
        there = pl.ds(pl.multiple_of(i * step_rows, step_rows), step_rows)
        return pltpu.make_async_remote_copy(
            src_ref=origin, dst_ref=cols.at[there], send_sem=col_send.at[0],
            recv_sem=col_recv.at[i], device_id=(row + 1, col), device_id_type=MESH,
        )

    def send_rows(tree, i, source):
        for link in range(3):
            @pl.when(links[tree][link][0])
            def _():
                row_copy(tree, link, i, source).start()

        @pl.when((row == owner) & (side == tree) & (row + 1 < row_devices))
        def _():
            here = row_slice(tree, i)
            origin = cov_ref.at[here, pl.ds(0, lead)] if source else rows.at[here]
            col_copy(i, origin).start()

    def head_slice(tree, p):
        return pl.ds(pl.multiple_of(p * NB + tree * part, part), part)

    def head_copy(tree, link, p):
        here = head_slice(tree, p)
        return pltpu.make_async_remote_copy(
            src_ref=inverse.at[here], dst_ref=inverse.at[here],
            send_sem=head_send.at[tree, link], recv_sem=head_recv.at[tree, p],
            device_id=(row, links[tree][link][1]), device_id_type=MESH,
        )

    def down_copy(p):
        here = pl.ds(pl.multiple_of(p * NB, NB), NB)
        return pltpu.make_async_remote_copy(
            src_ref=inverse.at[here], dst_ref=inverse.at[here], send_sem=down_send.at[0],
            recv_sem=down_recv.at[p], device_id=(row + 1, col), device_id_type=MESH,
        )

    def send_tree(tree, p):
        for link in range(3):
            @pl.when((row == 0) & links[tree][link][0])
            def _():
                head_copy(tree, link, p).start()

    def send_down(p):
        @pl.when(row + 1 < row_devices)
        def _():
            down_copy(p).start()

    own_rows = pltpu.make_async_copy(cov_ref.at[:, pl.ds(0, lead)], rows, local_sem.at[0])
    own_head = pltpu.make_async_copy(
        cov_ref.at[pl.ds(0, lead), pl.ds(0, lead)], factor, local_sem.at[1]
    )

    @pl.when(is_root)
    def _():
        own_head.start()

    @pl.when(is_source)
    def _():
        def first(i, carry):
            send_rows(0, i, True)
            send_rows(1, i, True)
            return carry

        lax.fori_loop(0, AHEAD, first, 0)
        own_rows.start()

    pace = CHUNKS // PANELS

    @pl.when(is_root)
    def _():
        own_head.wait()
        inverse[...] = jnp.zeros_like(inverse)
        below = lax.broadcasted_iota(jnp.int32, (NB, NB), 0)
        across = lax.broadcasted_iota(jnp.int32, (NB, NB), 1)
        for first in range(0, lead, NB):
            here = slice(first, first + NB)
            block = factor[here, here]
            block = jnp.where(below >= across, block, block.T)
            factor[here, here] = block + jnp.where(below == across, diag_ref[:, here], 0.0)
        for p in range(PANELS):
            def more(i, carry):
                send_rows(0, i, True)
                send_rows(1, i, True)
                return carry

            lax.fori_loop(
                min(CHUNKS, AHEAD + pace * p), min(CHUNKS, AHEAD + pace * (p + 1)), more, 0
            )
            factor_panel(factor, inverse, p * NB)
            send_tree(0, p)
            send_tree(1, p)
            send_down(p)

    @pl.when(jnp.logical_not(is_root))
    def _():
        lag = jnp.maximum(hops[0], hops[1]) + row
        head_start = pace + 4

        def step(t, carry):
            @pl.when(is_source & (t + AHEAD < CHUNKS))
            def _():
                send_rows(0, t + AHEAD, True)
                send_rows(1, t + AHEAD, True)

            for tree in range(2):
                i = t - SLACK * hops[tree]

                @pl.when(jnp.logical_not(is_source) & (i >= 0) & (i < CHUNKS))
                def _():
                    row_copy(tree, 0, i, False).wait_recv()
                    send_rows(tree, i, False)

            j = t - SLACK * (chain_hops + row - owner)

            @pl.when((row > owner) & (j >= 0) & (j < CHUNKS))
            def _():
                there = pl.ds(pl.multiple_of(j * step_rows, step_rows), step_rows)
                copy = col_copy(j, cols.at[there])
                copy.wait_recv()

                @pl.when(row + 1 < row_devices)
                def _():
                    copy.start()

            for tree in range(2):
                since = t - head_start - SLACK * hops[tree]
                p = since // pace

                @pl.when((row == 0) & (since >= 0) & (lax.rem(since, pace) == 0) & (p < PANELS))
                def _():
                    head_copy(tree, 0, p).wait_recv()
                    send_tree(tree, p)

            since = t - head_start - SLACK * lag
            p = since // pace

            @pl.when((since >= 0) & (lax.rem(since, pace) == 0) & (p < PANELS))
            def _():
                @pl.when(row > 0)
                def _():
                    down_copy(p).wait_recv()

                send_down(p)

            return carry

        longest = SLACK * (width + depth + 1 + row_devices)
        lax.fori_loop(0, CHUNKS + pace + 8 + longest, step, 0)

    @pl.when(is_source)
    def _():
        own_rows.wait()

    outputs = [
        pltpu.make_async_copy(rows, rows_out, local_sem.at[2]),
        pltpu.make_async_copy(inverse, inverse_out, local_sem.at[3]),
    ]
    for copy in outputs:
        copy.start()

    @pl.when(row > owner)
    def _():
        pltpu.make_async_copy(cols, cols_out, local_sem.at[4]).start()

    @pl.when(row == owner)
    def _():
        here = pl.ds(pl.multiple_of(side * half, half), half)
        pltpu.make_async_copy(rows.at[here], cols_out, local_sem.at[4]).start()

    @pl.when(is_root)
    def _():
        copy = pltpu.make_async_copy(factor, factor_out, local_sem.at[5])
        copy.start()
        copy.wait()

    for copy in outputs:
        copy.wait()

    @pl.when(row >= owner)
    def _():
        pltpu.make_async_copy(cols, cols_out, local_sem.at[4]).wait()

    for tree in range(2):
        for link in range(3):
            @pl.when(links[tree][link][0])
            def _():
                block = rows.at[pl.ds(0, half)]
                pltpu.make_async_remote_copy(
                    src_ref=block, dst_ref=block, send_sem=row_send.at[tree, link],
                    recv_sem=row_recv.at[tree, 0], device_id=(row, links[tree][link][1]),
                    device_id_type=MESH,
                ).wait_send()

            @pl.when((row == 0) & links[tree][link][0])
            def _():
                block = inverse.at[pl.ds(0, lead // 2)]
                pltpu.make_async_remote_copy(
                    src_ref=block, dst_ref=block, send_sem=head_send.at[tree, link],
                    recv_sem=head_recv.at[tree, 0], device_id=(row, links[tree][link][1]),
                    device_id_type=MESH,
                ).wait_send()

    @pl.when((row >= owner) & (row + 1 < row_devices))
    def _():
        pltpu.make_async_remote_copy(
            src_ref=cols, dst_ref=cols, send_sem=col_send.at[0], recv_sem=col_recv.at[0],
            device_id=(row + 1, col), device_id_type=MESH,
        ).wait_send()

    @pl.when(row + 1 < row_devices)
    def _():
        pltpu.make_async_remote_copy(
            src_ref=inverse, dst_ref=inverse, send_sem=down_send.at[0],
            recv_sem=down_recv.at[0], device_id=(row + 1, col), device_id_type=MESH,
        ).wait_send()


def spread(covariance, lead_diag, row_devices, col_devices):
    tile_rows, tile_cols = covariance.shape
    assert tile_rows == 2 * tile_cols
    lead = lead_diag.shape[0]
    width = max(1, row_devices // 2)
    dma = pltpu.SemaphoreType.DMA
    f32 = jnp.float32
    return pl.pallas_call(
        functools.partial(spread_kernel, row_devices, col_devices, width),
        out_shape=(
            jax.ShapeDtypeStruct((tile_rows, lead), f32),
            jax.ShapeDtypeStruct((tile_cols, lead), f32),
            jax.ShapeDtypeStruct((lead, lead), f32),
            jax.ShapeDtypeStruct((lead, lead), f32),
        ),
        in_specs=[ANY, VMEM],
        out_specs=(ANY,) * 4,
        scratch_shapes=[
            pltpu.VMEM((tile_rows, lead), f32),
            pltpu.VMEM((tile_cols, lead), f32),
            pltpu.VMEM((lead, lead), f32),
            pltpu.VMEM((lead, lead), f32),
            dma((6,)),
            dma((2, 3)),
            dma((2, CHUNKS)),
            dma((1,)),
            dma((CHUNKS,)),
            dma((2, 3)),
            dma((2, PANELS)),
            dma((1,)),
            dma((PANELS,)),
        ],
        compiler_params=pltpu.CompilerParams(
            has_side_effects=True, vmem_limit_bytes=50 * 1024 * 1024
        ),
        cost_estimate=pl.CostEstimate(flops=10**11, bytes_accessed=10**8, transcendentals=0),
    )(covariance, lead_diag.reshape(1, lead))


def on_device(covariance, weights, dual_slacks, returns, targets, sector_duals, lengths):
    tile_rows, tile_cols = covariance.shape
    row_devices, col_devices = lax.axis_size("row"), lax.axis_size("col")
    order_total = tile_rows * row_devices
    row_id = lax.axis_index("row")
    col_id = lax.axis_index("col")
    row_start = row_id * tile_rows
    col_start = col_id * tile_cols
    sectors_here = targets.shape[0]
    lead = PANELS * NB

    stacked = jnp.stack([weights, dual_slacks, returns])
    gathered = gather_small(stacked, row_devices, col_devices)
    full = gathered.transpose(1, 0, 2).reshape(3, order_total)
    full_weights, full_slacks, full_returns = full[0], full[1], full[2]
    full_diag = full_slacks / full_weights

    global_rows = row_start + jnp.arange(tile_rows, dtype=jnp.int32)
    global_cols = col_start + jnp.arange(tile_cols, dtype=jnp.int32)
    lower_mask = global_rows[:, None] >= global_cols[None, :]
    strict_mask = global_rows[:, None] > global_cols[None, :]
    weight_rows = lax.dynamic_slice_in_dim(full_weights, row_start, tile_rows)
    weight_cols = lax.dynamic_slice_in_dim(full_weights, col_start, tile_cols)
    row_part = jnp.sum(jnp.where(lower_mask, covariance * weight_cols[None, :], 0.0), axis=1)
    col_part = jnp.sum(jnp.where(strict_mask, covariance * weight_rows[:, None], 0.0), axis=0)
    product = sum_parts(row_part, col_part, row_devices, col_devices)

    rows_raw, cols_raw, factor, inverse = spread(
        covariance, full_diag[:lead], row_devices, col_devices
    )

    sector_ends = jnp.cumsum(lengths)
    offsets = sector_ends - lengths
    mean_gap = jnp.sum(full_weights * full_slacks) / order_total
    sector_first = col_id * sectors_here
    local_offsets = lax.dynamic_slice_in_dim(offsets, sector_first, sectors_here)
    local_ends = lax.dynamic_slice_in_dim(sector_ends, sector_first, sectors_here)
    sector_sizes = lax.dynamic_slice_in_dim(lengths, sector_first, sectors_here).astype(jnp.float32)
    all_assets = jnp.arange(order_total, dtype=jnp.int32)
    column_member = (all_assets[None, :] >= local_offsets[:, None]) & (
        all_assets[None, :] < local_ends[:, None]
    )
    held = jnp.sum(jnp.where(column_member, full_weights[None, :], 0.0), axis=1)
    sector_resid = targets - held / sector_sizes

    def right_sides(start, size):
        index = start + jnp.arange(size, dtype=jnp.int32)
        cut = lambda value: lax.dynamic_slice_in_dim(value, start, size)
        member = (index[:, None] >= offsets[None, :]) & (index[:, None] < sector_ends[None, :])
        prices = jnp.sum(jnp.where(member, sector_duals[None, :], 0.0), axis=1)
        rhs = cut(full_returns) - cut(product) - prices + SIGMA_GAP * mean_gap / cut(full_weights)
        local = (index[:, None] >= local_offsets[None, :]) & (index[:, None] < local_ends[None, :])
        columns = local.astype(jnp.float32) * lax.rsqrt(sector_sizes)[None, :]
        return jnp.concatenate([rhs[:, None], columns], axis=1)

    head_sides = right_sides(0, lead)
    extras = right_sides(row_start, tile_rows)

    solved_head = jnp.dot(inverse, head_sides, precision=HIGHEST)
    back_head = lax.dot_general(inverse, solved_head, (((0,), (0,)), ((), ())), precision=HIGHEST)
    cols_factor = lax.dot_general(cols_raw, inverse, NT, precision=HIGH)
    other = jnp.dot(cols_factor, inverse, precision=HIGH)
    lead_col = (global_cols < lead)[:, None]
    other = jnp.where(lead_col, -jnp.pad(inverse, ((0, tile_cols - lead), (0, 0))), other)

    update = lax.dot_general(rows_raw, other, NT, precision=HIGH)
    diag_rows = lax.dynamic_slice_in_dim(full_diag, row_start, tile_rows)
    on_diagonal = global_rows[:, None] == global_cols[None, :]
    base = jnp.where((global_cols < lead)[None, :], 0.0, covariance)
    base = base + jnp.where(
        on_diagonal & (global_cols >= lead)[None, :], diag_rows[:, None], 0.0
    )
    work = base - update
    lead_part = jnp.pad(factor, ((0, tile_rows - lead), (0, tile_cols - lead)))
    in_head = (global_rows < lead)[:, None] & (global_cols < lead)[None, :]
    work = jnp.where(in_head, lead_part, work)
    factored = jnp.where(lower_mask, work, 0.0)

    extras = extras - jnp.dot(rows_raw, back_head, precision=HIGH)
    top = jnp.where(row_id == 0, solved_head, extras[:lead])
    extras = lax.dynamic_update_slice_in_dim(extras, top, 0, 0)
    return (factored, extras[:, 0], extras[:, 1:], sector_resid)


def solution(mesh):
    return jax.shard_map(
        on_device,
        mesh=mesh,
        in_specs=(
            P("row", "col"),
            P(("row", "col")),
            P(("row", "col")),
            P(("row", "col")),
            P("col"),
            P(),
            P(),
        ),
        out_specs=(P("row", "col"), P("row"), P("row", "col"), P("col")),
        check_vma=False,
    )
```

```python
import functools

import jax
import jax.numpy as jnp
from jax import lax
from jax.experimental import pallas as pl
from jax.experimental.pallas import tpu as pltpu
from jax.sharding import PartitionSpec as P

NB = 128
PANELS = 8
CHUNKS = 64
SLACK = 4
AHEAD = 16
PACE = 6
ROOT_AHEAD = 8
ROOT_SHARE = 6
GROUP = 8
GROUPS = 8

HIGHEST = lax.Precision.HIGHEST
HIGH = lax.Precision.HIGH
SIGMA_GAP = 0.5
NT = (((1,), (1,)), ((), ()))
MESH = pl.DeviceIdType.MESH
VMEM = pl.BlockSpec(memory_space=pltpu.VMEM)
ANY = pl.BlockSpec(memory_space=pl.ANY)


def eliminate(block, work):
    width = block.shape[0]
    below = lax.broadcasted_iota(jnp.int32, (width, width), 0)
    across = lax.broadcasted_iota(jnp.int32, (width, width), 1)
    work[:, :width] = block
    work[:, width:] = (below == across).astype(jnp.float32)
    lanes = lax.broadcasted_iota(jnp.int32, (GROUP, width), 1)
    place = lax.broadcasted_iota(jnp.int32, (GROUP, 1), 0)
    rows = lax.broadcasted_iota(jnp.int32, (width, 2 * width), 0)

    def step(b, carry):
        base = pl.multiple_of(b * GROUP, GROUP)
        piece = work[pl.ds(base, GROUP), :]
        left = piece[:, :width]
        small = [
            jnp.sum(jnp.where(lanes == base + k, left, 0.0), axis=1, keepdims=True)
            for k in range(GROUP)
        ]
        for k in range(GROUP):
            pivot = small[k][k:k + 1]
            scale = lax.rsqrt(pivot)
            scale = scale * (1.5 - 0.5 * pivot * scale * scale)
            row = piece[k:k + 1] * scale
            factor = jnp.where(place > k, small[k] * scale, 0.0)
            piece = jnp.where(place == k, row, piece - factor * row)
            for other in range(k + 1, GROUP):
                small[other] = small[other] - factor * (small[other][k:k + 1] * scale)
        work[pl.ds(base, GROUP), :] = piece
        change = lax.dot_general(
            piece[:, :width], piece, (((0,), (0,)), ((), ())), precision=HIGHEST,
            preferred_element_type=jnp.float32,
        )
        work[...] = work[...] - jnp.where(rows >= base + GROUP, change, 0.0)
        return carry

    lax.fori_loop(0, width // GROUP, step, 0)
    upper = jnp.where(across >= below, work[:, :width], 0.0)
    return (upper.T, work[:, width:])


def factor_panel(factor_ref, inverse_ref, work_ref, first):
    order = factor_ref.shape[0]
    last = first + NB
    here = slice(first, last)
    lower, inverse = eliminate(factor_ref[here, here], work_ref)
    factor_ref[here, here] = lower
    inverse_ref[here, here] = inverse
    if first:
        done = jnp.dot(
            factor_ref[here, :first], inverse_ref[:first, :first], precision=HIGHEST,
            preferred_element_type=jnp.float32,
        )
        inverse_ref[here, :first] = -jnp.dot(
            inverse, done, precision=HIGHEST, preferred_element_type=jnp.float32
        )
    if last < order:
        below = lax.dot_general(
            factor_ref[last:, here], inverse, NT, precision=HIGHEST,
            preferred_element_type=jnp.float32,
        )
        factor_ref[last:, here] = below
        factor_ref[here, last:] = jnp.zeros((NB, order - last), jnp.float32)
        for top in range(last, order, NB):
            factor_ref[top:, top:top + NB] -= lax.dot_general(
                below[top - last:], below[top - last:top - last + NB], NT,
                precision=HIGHEST, preferred_element_type=jnp.float32,
            )


def gather_kernel(row_devices, col_devices, mine_ref, all_ref, send_sem, recv_sem):
    count = row_devices * col_devices
    me = lax.axis_index("row") * col_devices + lax.axis_index("col")
    all_ref[me] = mine_ref[...]

    def copy(k):
        target = lax.rem(me + k, count)
        return pltpu.make_async_remote_copy(
            src_ref=mine_ref, dst_ref=all_ref.at[me], send_sem=send_sem.at[k],
            recv_sem=recv_sem.at[k],
            device_id=(target // col_devices, lax.rem(target, col_devices)),
            device_id_type=MESH,
        )

    def start(k, carry):
        copy(k).start()
        return carry

    def finish(k, carry):
        copy(k).wait_recv()
        copy(k).wait_send()
        return carry

    lax.fori_loop(1, count, start, 0)
    lax.fori_loop(1, count, finish, 0)


def gather_small(mine, row_devices, col_devices):
    count = row_devices * col_devices
    return pl.pallas_call(
        functools.partial(gather_kernel, row_devices, col_devices),
        out_shape=jax.ShapeDtypeStruct((count,) + mine.shape, jnp.float32),
        in_specs=[VMEM],
        out_specs=VMEM,
        scratch_shapes=[pltpu.SemaphoreType.DMA((count,)), pltpu.SemaphoreType.DMA((count,))],
        compiler_params=pltpu.CompilerParams(has_side_effects=True),
        cost_estimate=pl.CostEstimate(flops=10**9, bytes_accessed=10**6, transcendentals=0),
    )(mine)


def sum_kernel(
    row_devices, col_devices, per_col, row_ref, col_ref, all_ref, inbox, mine, send_sem,
    recv_sem, send_back, recv_back,
):
    count = row_devices * col_devices
    row, col = lax.axis_index("row"), lax.axis_index("col")
    me = row * col_devices + col

    def to_row(s):
        return pltpu.make_async_remote_copy(
            src_ref=row_ref.at[s], dst_ref=inbox.at[col], send_sem=send_sem.at[s],
            recv_sem=recv_sem.at[col], device_id=(row, s), device_id_type=MESH,
        )

    def to_col(t):
        target = col * per_col + t
        return target, pltpu.make_async_remote_copy(
            src_ref=col_ref.at[t], dst_ref=inbox.at[col_devices + row],
            send_sem=send_sem.at[col_devices + t], recv_sem=recv_sem.at[col_devices + row],
            device_id=(target // col_devices, lax.rem(target, col_devices)),
            device_id_type=MESH,
        )

    def arrival(slot):
        return pltpu.make_async_remote_copy(
            src_ref=inbox.at[slot], dst_ref=inbox.at[slot], send_sem=send_sem.at[0],
            recv_sem=recv_sem.at[slot], device_id=(row, col), device_id_type=MESH,
        )

    inbox[col] = row_ref[col]
    for s in range(col_devices):
        @pl.when(s != col)
        def _():
            to_row(s).start()
    for t in range(per_col):
        target, copy = to_col(t)

        @pl.when(target != me)
        def _():
            copy.start()

        @pl.when(target == me)
        def _():
            inbox[col_devices + row] = col_ref[t]
    source_col = me // per_col
    for s in range(col_devices):
        @pl.when(s != col)
        def _():
            arrival(s).wait_recv()
    for q in range(row_devices):
        @pl.when(q * col_devices + source_col != me)
        def _():
            arrival(col_devices + q).wait_recv()
    total = inbox[0]
    for slot in range(1, col_devices + row_devices):
        total = total + inbox[slot]
    mine[...] = total
    all_ref[me] = total

    def back(k):
        target = lax.rem(me + k, count)
        return pltpu.make_async_remote_copy(
            src_ref=mine, dst_ref=all_ref.at[me], send_sem=send_back.at[k],
            recv_sem=recv_back.at[k],
            device_id=(target // col_devices, lax.rem(target, col_devices)),
            device_id_type=MESH,
        )

    def start(k, carry):
        back(k).start()
        return carry

    def finish(k, carry):
        back(k).wait_recv()
        back(k).wait_send()
        return carry

    lax.fori_loop(1, count, start, 0)
    lax.fori_loop(1, count, finish, 0)
    for s in range(col_devices):
        @pl.when(s != col)
        def _():
            to_row(s).wait_send()
    for t in range(per_col):
        target, copy = to_col(t)

        @pl.when(target != me)
        def _():
            copy.wait_send()


def sum_parts(row_part, col_part, row_devices, col_devices):
    count = row_devices * col_devices
    piece = row_part.shape[0] // col_devices
    per_col = col_part.shape[0] // piece
    dma = pltpu.SemaphoreType.DMA
    return pl.pallas_call(
        functools.partial(sum_kernel, row_devices, col_devices, per_col),
        out_shape=jax.ShapeDtypeStruct((count, 1, piece), jnp.float32),
        in_specs=[VMEM, VMEM],
        out_specs=VMEM,
        scratch_shapes=[
            pltpu.VMEM((col_devices + row_devices, 1, piece), jnp.float32),
            pltpu.VMEM((1, piece), jnp.float32),
            dma((col_devices + per_col,)),
            dma((col_devices + row_devices,)),
            dma((count,)),
            dma((count,)),
        ],
        compiler_params=pltpu.CompilerParams(has_side_effects=True),
        cost_estimate=pl.CostEstimate(flops=10**9, bytes_accessed=10**6, transcendentals=0),
    )(row_part.reshape(col_devices, 1, piece), col_part.reshape(per_col, 1, piece)).reshape(-1)


def spread_kernel(
    row_devices, col_devices, width, cov_ref, diag_ref, rows_out, other_out, factor_out,
    inverse_out, both_out, rows, cols, factor, inverse, both, other, stage, work, local_sem, row_send, row_recv, col_send,
    col_recv, head_send, head_recv, down_send, down_recv,
):
    tile_rows, lead = rows.shape
    depth = col_devices // width
    half = tile_rows // 2
    step_rows = half // CHUNKS
    part = NB // 2
    group_rows = half // GROUPS
    row, col = lax.axis_index("row"), lax.axis_index("col")
    z, x = col // width, lax.rem(col, width)
    owner = col // 2
    side = lax.rem(col, 2)
    is_source = col == 0
    is_root = is_source & (row == 0)

    links = (
        (
            ((z == 0) & (x + 1 < width), col + 1),
            ((x >= 1) & (z + 1 < depth), col + width),
            ((z >= 1) & (x == 1), col - 1),
        ),
        (
            ((x == 0) & (z + 1 < depth), col + width),
            ((z >= 1) & (x + 1 < width), col + 1),
            ((z == 1) & (x >= 1), col - width),
        ),
    )
    hops = (
        jnp.where(x >= 1, x + z, jnp.where(z >= 1, z + 2, 0)),
        jnp.where(z >= 1, x + z, jnp.where(x >= 1, x + 2, 0)),
    )
    chain_hops = jnp.where(side == 0, hops[0], hops[1])

    def row_slice(tree, i):
        return pl.ds(pl.multiple_of(tree * half + i * step_rows, step_rows), step_rows)

    def row_copy(tree, link, i, source):
        here = row_slice(tree, i)
        origin = cov_ref.at[here, pl.ds(0, lead)] if source else rows.at[here]
        return pltpu.make_async_remote_copy(
            src_ref=origin, dst_ref=rows.at[here], send_sem=row_send.at[tree, link],
            recv_sem=row_recv.at[tree, i], device_id=(row, links[tree][link][1]),
            device_id_type=MESH,
        )

    def col_copy(i, origin):
        there = pl.ds(pl.multiple_of(i * step_rows, step_rows), step_rows)
        return pltpu.make_async_remote_copy(
            src_ref=origin, dst_ref=cols.at[there], send_sem=col_send.at[0],
            recv_sem=col_recv.at[i], device_id=(row + 1, col), device_id_type=MESH,
        )

    def send_rows(tree, i, source):
        for link in range(3):
            @pl.when(links[tree][link][0])
            def _():
                row_copy(tree, link, i, source).start()

        @pl.when((row == owner) & (side == tree) & (row + 1 < row_devices))
        def _():
            here = row_slice(tree, i)
            origin = cov_ref.at[here, pl.ds(0, lead)] if source else rows.at[here]
            col_copy(i, origin).start()

    def head_slice(tree, p):
        return pl.ds(pl.multiple_of(p * NB + tree * part, part), part)

    def head_copy(tree, link, p):
        here = head_slice(tree, p)
        return pltpu.make_async_remote_copy(
            src_ref=inverse.at[here], dst_ref=inverse.at[here],
            send_sem=head_send.at[tree, link], recv_sem=head_recv.at[tree, p],
            device_id=(row, links[tree][link][1]), device_id_type=MESH,
        )

    def down_copy(p):
        here = pl.ds(pl.multiple_of(p * NB, NB), NB)
        return pltpu.make_async_remote_copy(
            src_ref=inverse.at[here], dst_ref=inverse.at[here], send_sem=down_send.at[0],
            recv_sem=down_recv.at[p], device_id=(row + 1, col), device_id_type=MESH,
        )

    def send_tree(tree, p):
        for link in range(3):
            @pl.when((row == 0) & links[tree][link][0])
            def _():
                head_copy(tree, link, p).start()

    def send_down(p):
        @pl.when(row + 1 < row_devices)
        def _():
            down_copy(p).start()

    def keep_rows(here):
        pltpu.make_async_copy(rows.at[here], rows_out.at[here], local_sem.at[2]).start()

    def keep_head(p):
        here = pl.ds(pl.multiple_of(p * NB, NB), NB)
        pltpu.make_async_copy(inverse.at[here], inverse_out.at[here], local_sem.at[3]).start()

    def keep_own():
        own_rows.wait()
        keep_rows(pl.ds(0, tile_rows))

    def add_both(p):
        here = pl.ds(pl.multiple_of(p * NB, NB), NB)

        def add(k, carry):
            there = pl.ds(pl.multiple_of(k * NB, NB), NB)
            both[there, :] += lax.dot_general(
                inverse[here, there], inverse[here, :], (((0,), (0,)), ((), ())),
                precision=HIGHEST, preferred_element_type=jnp.float32,
            )
            return carry

        lax.fori_loop(0, lead // NB, add, 0)

    def other_group(g):
        start = pl.multiple_of(g * group_rows, group_rows)
        there = pl.ds(start, group_rows)
        direct = is_source & (start < lead)

        @pl.when(direct)
        def _():
            other[there, :] = -inverse[there, :]

        @pl.when(jnp.logical_not(direct))
        def _():
            @pl.when(row == owner)
            def _():
                begin = pl.multiple_of(side * half + g * group_rows, group_rows)
                stage[...] = rows[pl.ds(begin, group_rows), :]

            @pl.when(row > owner)
            def _():
                stage[...] = cols[there, :]

            def part_of(k, carry):
                lanes = pl.ds(pl.multiple_of(k * 2 * NB, 2 * NB), 2 * NB)
                other[there, lanes] = jnp.dot(
                    stage[...], both[:, lanes], precision=HIGHEST,
                    preferred_element_type=jnp.float32,
                )
                return carry

            lax.fori_loop(0, lead // (2 * NB), part_of, 0)

        pltpu.make_async_copy(other.at[there], other_out.at[there], local_sem.at[4]).start()

    own_rows = pltpu.make_async_copy(cov_ref.at[:, pl.ds(0, lead)], rows, local_sem.at[0])
    own_head = pltpu.make_async_copy(
        cov_ref.at[pl.ds(0, lead), pl.ds(0, lead)], factor, local_sem.at[1]
    )

    @pl.when(is_root)
    def _():
        own_head.start()

    @pl.when(is_source)
    def _():
        def first(i, carry):
            send_rows(0, i, True)
            send_rows(1, i, True)
            return carry

        lax.fori_loop(0, jnp.where(row == 0, ROOT_AHEAD, AHEAD), first, 0)
        own_rows.start()

    pace = PACE
    both[...] = jnp.zeros_like(both)

    @pl.when(is_root)
    def _():
        own_head.wait()
        keep_own()
        inverse[...] = jnp.zeros_like(inverse)
        below = lax.broadcasted_iota(jnp.int32, (NB, NB), 0)
        across = lax.broadcasted_iota(jnp.int32, (NB, NB), 1)
        for first in range(0, lead, NB):
            here = slice(first, first + NB)
            block = factor[here, here]
            block = jnp.where(below >= across, block, block.T)
            factor[here, here] = block + jnp.where(below == across, diag_ref[:, here], 0.0)
        def more(i, carry):
            send_rows(0, i, True)
            send_rows(1, i, True)
            return carry

        sent = ROOT_AHEAD
        for p in range(PANELS):
            factor_panel(factor, inverse, work, p * NB)
            send_tree(0, p)
            send_tree(1, p)
            send_down(p)
            keep_head(p)
            following = CHUNKS if p + 1 == PANELS else min(CHUNKS, sent + ROOT_SHARE)
            lax.fori_loop(sent, following, more, 0)
            sent = following

        def add_all(p, carry):
            add_both(p)
            return carry

        def group_all(g, carry):
            other_group(g)
            return carry

        lax.fori_loop(0, PANELS, add_all, 0)
        lax.fori_loop(0, GROUPS, group_all, 0)

    @pl.when(jnp.logical_not(is_root))
    def _():
        lag = jnp.maximum(hops[0], hops[1]) + row
        head_start = pace + 4

        @pl.when(is_source)
        def _():
            keep_own()


        def step(t, carry):
            @pl.when(is_source & (t + AHEAD < CHUNKS))
            def _():
                send_rows(0, t + AHEAD, True)
                send_rows(1, t + AHEAD, True)

            for tree in range(2):
                i = t - SLACK * hops[tree]

                @pl.when(jnp.logical_not(is_source) & (i >= 0) & (i < CHUNKS))
                def _():
                    row_copy(tree, 0, i, False).wait_recv()
                    send_rows(tree, i, False)
                    keep_rows(row_slice(tree, i))

            j = t - SLACK * (chain_hops + row - owner)

            @pl.when((row > owner) & (j >= 0) & (j < CHUNKS))
            def _():
                there = pl.ds(pl.multiple_of(j * step_rows, step_rows), step_rows)
                copy = col_copy(j, cols.at[there])
                copy.wait_recv()

                @pl.when(row + 1 < row_devices)
                def _():
                    copy.start()

            for tree in range(2):
                since = t - head_start - SLACK * hops[tree]
                p = since // pace

                @pl.when((row == 0) & (since >= 0) & (lax.rem(since, pace) == 0) & (p < PANELS))
                def _():
                    head_copy(tree, 0, p).wait_recv()
                    send_tree(tree, p)

            since = t - head_start - SLACK * lag
            p = since // pace

            @pl.when((since >= 0) & (lax.rem(since, pace) == 0) & (p < PANELS))
            def _():
                @pl.when(row > 0)
                def _():
                    down_copy(p).wait_recv()

                send_down(p)
                keep_head(p)
                add_both(p)

            def grouped(g, inner):
                arrived = (g + 1) * (CHUNKS // GROUPS) + SLACK * (chain_hops + row - owner)
                solved = head_start + SLACK * lag + pace * (PANELS - 1) + g + 1

                @pl.when((row >= owner) & (t == jnp.maximum(arrived, solved)))
                def _():
                    other_group(g)

                return inner

            lax.fori_loop(0, GROUPS, grouped, 0)
            return carry

        longest = SLACK * (width + depth + 1 + row_devices)
        lax.fori_loop(0, max(CHUNKS, pace * PANELS) + pace + 8 + longest, step, 0)

    @pl.when(is_root)
    def _():
        copy = pltpu.make_async_copy(factor, factor_out, local_sem.at[5])
        copy.start()
        copy.wait()

    pltpu.make_async_copy(rows, rows_out, local_sem.at[2]).wait()
    pltpu.make_async_copy(inverse, inverse_out, local_sem.at[3]).wait()
    keep_both = pltpu.make_async_copy(both, both_out, local_sem.at[6])
    keep_both.start()
    keep_both.wait()

    @pl.when(row >= owner)
    def _():
        pltpu.make_async_copy(other, other_out, local_sem.at[4]).wait()

    for tree in range(2):
        for link in range(3):
            @pl.when(links[tree][link][0])
            def _():
                block = rows.at[pl.ds(0, half)]
                pltpu.make_async_remote_copy(
                    src_ref=block, dst_ref=block, send_sem=row_send.at[tree, link],
                    recv_sem=row_recv.at[tree, 0], device_id=(row, links[tree][link][1]),
                    device_id_type=MESH,
                ).wait_send()

            @pl.when((row == 0) & links[tree][link][0])
            def _():
                block = inverse.at[pl.ds(0, lead // 2)]
                pltpu.make_async_remote_copy(
                    src_ref=block, dst_ref=block, send_sem=head_send.at[tree, link],
                    recv_sem=head_recv.at[tree, 0], device_id=(row, links[tree][link][1]),
                    device_id_type=MESH,
                ).wait_send()

    @pl.when((row >= owner) & (row + 1 < row_devices))
    def _():
        pltpu.make_async_remote_copy(
            src_ref=cols, dst_ref=cols, send_sem=col_send.at[0], recv_sem=col_recv.at[0],
            device_id=(row + 1, col), device_id_type=MESH,
        ).wait_send()

    @pl.when(row + 1 < row_devices)
    def _():
        pltpu.make_async_remote_copy(
            src_ref=inverse, dst_ref=inverse, send_sem=down_send.at[0],
            recv_sem=down_recv.at[0], device_id=(row + 1, col), device_id_type=MESH,
        ).wait_send()


def spread(covariance, lead_diag, row_devices, col_devices):
    tile_rows, tile_cols = covariance.shape
    assert tile_rows == 2 * tile_cols
    lead = lead_diag.shape[0]
    width = max(1, row_devices // 2)
    dma = pltpu.SemaphoreType.DMA
    f32 = jnp.float32
    return pl.pallas_call(
        functools.partial(spread_kernel, row_devices, col_devices, width),
        out_shape=(
            jax.ShapeDtypeStruct((tile_rows, lead), f32),
            jax.ShapeDtypeStruct((tile_cols, lead), f32),
            jax.ShapeDtypeStruct((lead, lead), f32),
            jax.ShapeDtypeStruct((lead, lead), f32),
            jax.ShapeDtypeStruct((lead, lead), f32),
        ),
        in_specs=[ANY, VMEM],
        out_specs=(ANY,) * 5,
        scratch_shapes=[
            pltpu.VMEM((tile_rows, lead), f32),
            pltpu.VMEM((tile_cols, lead), f32),
            pltpu.VMEM((lead, lead), f32),
            pltpu.VMEM((lead, lead), f32),
            pltpu.VMEM((lead, lead), f32),
            pltpu.VMEM((tile_cols, lead), f32),
            pltpu.VMEM((tile_cols // GROUPS, lead), f32),
            pltpu.VMEM((NB, 2 * NB), f32),
            dma((7,)),
            dma((2, 3)),
            dma((2, CHUNKS)),
            dma((1,)),
            dma((CHUNKS,)),
            dma((2, 3)),
            dma((2, PANELS)),
            dma((1,)),
            dma((PANELS,)),
        ],
        compiler_params=pltpu.CompilerParams(
            has_side_effects=True, vmem_limit_bytes=58 * 1024 * 1024
        ),
        cost_estimate=pl.CostEstimate(flops=10**11, bytes_accessed=10**8, transcendentals=0),
    )(covariance, lead_diag.reshape(1, lead))


def on_device(covariance, weights, dual_slacks, returns, targets, sector_duals, lengths):
    tile_rows, tile_cols = covariance.shape
    row_devices, col_devices = lax.axis_size("row"), lax.axis_size("col")
    order_total = tile_rows * row_devices
    row_id = lax.axis_index("row")
    col_id = lax.axis_index("col")
    row_start = row_id * tile_rows
    col_start = col_id * tile_cols
    sectors_here = targets.shape[0]
    lead = PANELS * NB

    stacked = jnp.stack([weights, dual_slacks, returns])
    gathered = gather_small(stacked, row_devices, col_devices)
    full = gathered.transpose(1, 0, 2).reshape(3, order_total)
    full_weights, full_slacks, full_returns = full[0], full[1], full[2]
    full_diag = full_slacks / full_weights

    global_rows = row_start + jnp.arange(tile_rows, dtype=jnp.int32)
    global_cols = col_start + jnp.arange(tile_cols, dtype=jnp.int32)
    lower_mask = global_rows[:, None] >= global_cols[None, :]
    strict_mask = global_rows[:, None] > global_cols[None, :]
    weight_rows = lax.dynamic_slice_in_dim(full_weights, row_start, tile_rows)
    weight_cols = lax.dynamic_slice_in_dim(full_weights, col_start, tile_cols)
    row_part = jnp.sum(jnp.where(lower_mask, covariance * weight_cols[None, :], 0.0), axis=1)
    col_part = jnp.sum(jnp.where(strict_mask, covariance * weight_rows[:, None], 0.0), axis=0)
    product = sum_parts(row_part, col_part, row_devices, col_devices)

    rows_raw, other, factor, inverse, both = spread(
        covariance, full_diag[:lead], row_devices, col_devices
    )

    sector_ends = jnp.cumsum(lengths)
    offsets = sector_ends - lengths
    mean_gap = jnp.sum(full_weights * full_slacks) / order_total
    sector_first = col_id * sectors_here
    local_offsets = lax.dynamic_slice_in_dim(offsets, sector_first, sectors_here)
    local_ends = lax.dynamic_slice_in_dim(sector_ends, sector_first, sectors_here)
    sector_sizes = lax.dynamic_slice_in_dim(lengths, sector_first, sectors_here).astype(jnp.float32)
    all_assets = jnp.arange(order_total, dtype=jnp.int32)
    column_member = (all_assets[None, :] >= local_offsets[:, None]) & (
        all_assets[None, :] < local_ends[:, None]
    )
    held = jnp.sum(jnp.where(column_member, full_weights[None, :], 0.0), axis=1)
    sector_resid = targets - held / sector_sizes

    def right_sides(start, size):
        index = start + jnp.arange(size, dtype=jnp.int32)
        cut = lambda value: lax.dynamic_slice_in_dim(value, start, size)
        member = (index[:, None] >= offsets[None, :]) & (index[:, None] < sector_ends[None, :])
        prices = jnp.sum(jnp.where(member, sector_duals[None, :], 0.0), axis=1)
        rhs = cut(full_returns) - cut(product) - prices + SIGMA_GAP * mean_gap / cut(full_weights)
        local = (index[:, None] >= local_offsets[None, :]) & (index[:, None] < local_ends[None, :])
        columns = local.astype(jnp.float32) * lax.rsqrt(sector_sizes)[None, :]
        return jnp.concatenate([rhs[:, None], columns], axis=1)

    head_sides = right_sides(0, lead)
    extras = right_sides(row_start, tile_rows)

    solved_head = jnp.dot(inverse, head_sides, precision=HIGH)
    back_head = jnp.dot(both, head_sides, precision=HIGH)

    update = lax.dot_general(rows_raw, other, NT, precision=HIGH)
    diag_rows = lax.dynamic_slice_in_dim(full_diag, row_start, tile_rows)
    on_diagonal = global_rows[:, None] == global_cols[None, :]
    base = jnp.where((global_cols < lead)[None, :], 0.0, covariance)
    base = base + jnp.where(
        on_diagonal & (global_cols >= lead)[None, :], diag_rows[:, None], 0.0
    )
    work = base - update
    lead_part = jnp.pad(factor, ((0, tile_rows - lead), (0, tile_cols - lead)))
    in_head = (global_rows < lead)[:, None] & (global_cols < lead)[None, :]
    work = jnp.where(in_head, lead_part, work)
    factored = jnp.where(lower_mask, work, 0.0)

    extras = extras - jnp.dot(rows_raw, back_head, precision=HIGH)
    top = jnp.where(row_id == 0, solved_head, extras[:lead])
    extras = lax.dynamic_update_slice_in_dim(extras, top, 0, 0)
    return (factored, extras[:, 0], extras[:, 1:], sector_resid)


def solution(mesh):
    return jax.shard_map(
        on_device,
        mesh=mesh,
        in_specs=(
            P("row", "col"),
            P(("row", "col")),
            P(("row", "col")),
            P(("row", "col")),
            P("col"),
            P(),
            P(),
        ),
        out_specs=(P("row", "col"), P("row"), P("row", "col"), P("col")),
        check_vma=False,
    )
```
